128 devices in a mesh: env: 128 (over z, x, y, core).
Axes of the slice: x: 4, y: 4, z: 4, core: 2. Of those that a mesh axis runs over, the one named last changes fastest.
Arguments:
- observations: bfloat16 [16, 2048, 96], P(None, 'env'), may hold values from -6 to 6
- physics_params: bfloat16 [2048, 32], P('env'), may hold values from -4 to 4
- actions: int32 [16, 2048, 20], P(None, 'env'), may hold values from 0 to 10
- reset_step: int32 [2048], P('env'), may hold values from 0 to 16
- hidden_start: bfloat16 [2048, 1024], P('env'), may hold values from -0.8984375 to 0.8984375
- cell_start: float32 [2048, 1024], P('env'), may hold values from -4 to 4
- old_logp: float32 [16, 2048], P(None, 'env'), may hold values from -50.5 to -47.5
- advantages: float32 [16, 2048], P(None, 'env'), may hold values from 3 to 7
- returns: float32 [16, 2048], P(None, 'env'), may hold values from -5 to 5
- lstm_weight: bfloat16 [1152, 4096], replicated, may hold values from -0.1875 to 0.1875
- lstm_bias: float32 [4096], replicated, may hold values from -4 to 4
- head_weight: bfloat16 [1024, 221], replicated, may hold values from -0.1875 to 0.1875
Outputs:
- lstm_step: float32 [1152, 4096], P('env')
- bias_step: float32 [4096], P('env')
- head_step: float32 [1024, 221], P('env')
- kl_mean: float32 [], replicated
The draws below stay inside these ranges and needn't reach their ends.
All inputs are finite; a program needn't handle non-finite values.
Results may differ from the reference program's by a relative error of at most 0.0073.
Values sent between devices are 32-bit elements; how exact they have to be, the bound alone decides.
No kernel may reach another device: no remote copies, remote signals or barrier semaphores. Data moves between devices by JAX's collectives and lax.ppermute only.
A program may use at most 128 MiB of HBM per device.

```python
import math
import jax
import jax.numpy as jnp
from jax import lax

H = 1024
OBS = 96
PHYS = 32
ACT = 20
BINS = 11
STEPS = 16
IN = 128
ENVS = 2048


def with_ends(entries, key, least, largest):
    extent = entries.shape
    spot = [jax.random.randint(jax.random.fold_in(key, axis), (), 0, extent[axis]) for axis in range(len(extent))]
    entries = entries.at[tuple(spot)].set(least)
    longest = extent.index(max(extent))
    spot[longest] = (spot[longest] + 1) % extent[longest]
    return entries.at[tuple(spot)].set(largest)


def shard_levels(stream_key, shape, pieces, low, high):
    level, own = 1.0, jax.random.fold_in(stream_key, 6)
    for position, parts in pieces:
        heights = jnp.exp(jax.random.uniform(jax.random.fold_in(own, position), (parts,), jnp.float32, low / len(pieces), high / len(pieces)))
        level = level * jnp.repeat(heights, shape[position] // parts).reshape([-1 if axis == position else 1 for axis in range(len(shape))])
    return level


def gaussian(rng, shape, scale, reach, cuts=(), kind=jnp.bfloat16):
    gain = shard_levels(rng, shape, cuts, -0.22, 0.18) if cuts else 1.0
    entries = jax.random.normal(rng, shape, jnp.float32) * scale * gain
    return jnp.minimum(jnp.maximum(entries, -reach), reach).astype(kind)


def setup_inputs(seed: int = 0) -> dict:
    streams_of = jax.random.split(jax.random.key(seed), 13)
    observations = gaussian(streams_of[0], (STEPS, ENVS, OBS), 1.0, 6.0, ((1, 128),))
    physics_params = gaussian(streams_of[1], (ENVS, PHYS), 1.0, 4.0, ((0, 128),))
    actions = with_ends(jax.random.randint(streams_of[2], (STEPS, ENVS, ACT), 0, BINS), jax.random.fold_in(streams_of[2], 1), 0, BINS - 1).astype(jnp.int32)
    reset_step = with_ends(jax.random.randint(streams_of[3], (ENVS,), 0, STEPS + 1), jax.random.fold_in(streams_of[3], 1), 0, STEPS).astype(jnp.int32)
    hidden_start = jnp.clip(jax.random.uniform(streams_of[4], (ENVS, H), jnp.float32, -0.8984375, 0.8984375) * shard_levels(streams_of[4], (ENVS, H), ((0, 128),), -0.4, 0.0), -0.8984375, 0.8984375).astype(jnp.bfloat16)
    cell_start = gaussian(streams_of[5], (ENVS, H), 1.0, 4.0, ((0, 128),), jnp.float32)
    old_logp = jnp.clip(-50.5 + 3.0 * jax.random.uniform(streams_of[6], (STEPS, ENVS), jnp.float32) ** shard_levels(streams_of[6], (STEPS, ENVS), ((1, 128),), -0.2, 0.2), -50.5, -47.5)
    advantages = jnp.clip(3.0 + 4.0 * jax.random.uniform(streams_of[7], (STEPS, ENVS), jnp.float32) ** shard_levels(streams_of[7], (STEPS, ENVS), ((1, 128),), -0.2, 0.2), 3.0, 7.0)
    returns = gaussian(streams_of[8], (STEPS, ENVS), 1.0, 5.0, ((1, 128),), jnp.float32)
    lstm_weight = gaussian(streams_of[9], (IN + H, 4 * H), (IN + H) ** -0.5, 0.1875)
    lstm_bias = gaussian(streams_of[10], (4 * H,), 1.0, 4.0, (), jnp.float32)
    head_weight = gaussian(streams_of[11], (H, ACT * BINS + 1), H ** -0.5, 0.1875)
    return dict(observations=observations, physics_params=physics_params, actions=actions, reset_step=reset_step, hidden_start=hidden_start, cell_start=cell_start, old_logp=old_logp, advantages=advantages, returns=returns, lstm_weight=lstm_weight, lstm_bias=lstm_bias, head_weight=head_weight)


kl_coef = 0.5
value_coef = 0.5
spread_floor = 0.25

def local_terms(observations, physics_params, actions, reset_step, hidden_start, cell_start, old_logp, norm_adv, returns, lstm_weight, lstm_bias, head_weight):
    step_count, env_count = (observations.shape[0], observations.shape[1])
    hidden = hidden_start.shape[1]
    width_in = lstm_weight.shape[0] - hidden
    act_count = actions.shape[2]
    bin_count = (head_weight.shape[1] - 1) // act_count
    phys_tiled = jnp.broadcast_to(physics_params[None], (step_count, env_count, physics_params.shape[1]))
    inputs = jnp.concatenate([observations, phys_tiled], axis=2).reshape(step_count * env_count, width_in)
    w_rec = lstm_weight[width_in:]
    projected = jnp.dot(inputs, lstm_weight[:width_in], preferred_element_type=jnp.float32) + lstm_bias
    projected = projected.reshape(step_count, env_count, 4 * hidden)
    columns = lax.broadcasted_iota(jnp.int32, (1, 4 * hidden), 1)
    is_cand = (columns >= 2 * hidden) & (columns < 3 * hidden)
    step_ids = jnp.arange(step_count, dtype=jnp.int32)

    def advance(state_pair, inputs_now):
        h_prev, c_prev = state_pair
        proj_now, step_index = inputs_now
        keep_mask = (reset_step != step_index)[:, None]
        h_kept = jnp.where(keep_mask, h_prev, jnp.zeros_like(h_prev))
        c_kept = jnp.where(keep_mask, c_prev, jnp.zeros_like(c_prev))
        pre_act = proj_now + jnp.dot(h_kept, w_rec, preferred_element_type=jnp.float32)
        activated = jnp.where(is_cand, jnp.tanh(pre_act), jax.nn.sigmoid(pre_act))
        gate_i = activated[:, :hidden]
        gate_f = activated[:, hidden:2 * hidden]
        cand_gate = activated[:, 2 * hidden:3 * hidden]
        gate_o = activated[:, 3 * hidden:]
        c_new = gate_f * c_kept + gate_i * cand_gate
        tanh_c = jnp.tanh(c_new)
        h_new = (gate_o * tanh_c).astype(jnp.bfloat16)
        return ((h_new, c_new), (h_kept, c_kept, activated, tanh_c, h_new))
    final_state, saved = lax.scan(advance, (hidden_start, cell_start), (projected, step_ids))
    h_kept_all, c_kept_all, activated_all, tanh_all, hseq = saved
    h_flat = hseq.reshape(step_count * env_count, hidden)
    logits = jnp.dot(h_flat, head_weight, preferred_element_type=jnp.float32)
    policy = logits[:, :act_count * bin_count].reshape(-1, act_count, bin_count)
    value_pred = logits[:, act_count * bin_count]
    exp_policy = jnp.exp(policy)
    sum_exp = lax.optimization_barrier(jnp.sum(exp_policy, axis=2, keepdims=True))
    soft_probs = exp_policy / sum_exp
    log_probs = policy - jnp.log(sum_exp)
    levels = lax.broadcasted_iota(jnp.int32, (1, 1, bin_count), 2)
    onehot = (actions.reshape(-1, act_count)[:, :, None] == levels).astype(jnp.float32)
    token_logp = lax.optimization_barrier(jnp.sum(onehot * log_probs, axis=(1, 2)))
    log_ratio = token_logp - old_logp.reshape(-1)
    prob_ratio = jnp.exp(log_ratio)
    kl_part = jnp.sum(prob_ratio - 1.0 - log_ratio)
    grad_logp = kl_coef * (prob_ratio - 1.0) - norm_adv.reshape(-1) * prob_ratio
    grad_policy = grad_logp[:, None, None] * (onehot - soft_probs)
    grad_value = value_coef * (value_pred - returns.reshape(-1))
    grad_logits = jnp.concatenate([grad_policy.reshape(-1, act_count * bin_count), grad_value[:, None]], axis=1).astype(jnp.bfloat16)
    head_grad = lax.dot_general(h_flat, grad_logits, (((0,), (0,)), ((), ())), preferred_element_type=jnp.float32)
    from_head = lax.dot_general(grad_logits, head_weight, (((1,), (1,)), ((), ())), preferred_element_type=jnp.float32)
    from_head = from_head.reshape(step_count, env_count, hidden)

    def retreat(state_pair, inputs_now):
        grad_h_next, grad_c_next = state_pair
        c_kept, activated, tanh_c, head_part, step_index = inputs_now
        keep_mask = (reset_step != step_index)[:, None]
        gate_i = activated[:, :hidden]
        gate_f = activated[:, hidden:2 * hidden]
        cand_gate = activated[:, 2 * hidden:3 * hidden]
        gate_o = activated[:, 3 * hidden:]
        grad_h = head_part + grad_h_next
        grad_c = grad_c_next + grad_h * gate_o * (1.0 - tanh_c * tanh_c)
        upstream = jnp.concatenate([grad_c * cand_gate, grad_c * c_kept, grad_c * gate_i, grad_h * tanh_c], axis=1)
        act_slope = jnp.where(is_cand, 1.0 - activated * activated, activated * (1.0 - activated))
        grad_gates = (upstream * act_slope).astype(jnp.bfloat16)
        grad_h_prev = lax.dot_general(grad_gates, w_rec, (((1,), (1,)), ((), ())), preferred_element_type=jnp.float32)
        grad_h_prev = jnp.where(keep_mask, grad_h_prev, jnp.zeros_like(grad_h_prev))
        grad_c_prev = jnp.where(keep_mask, grad_c * gate_f, jnp.zeros_like(grad_c))
        return ((grad_h_prev, grad_c_prev), grad_gates)
    zero_state = jnp.zeros((env_count, hidden), jnp.float32)
    final_grads, grad_gates = lax.scan(retreat, (zero_state, zero_state), (c_kept_all, activated_all, tanh_all, from_head, step_ids), reverse=True)
    operand = jnp.concatenate([inputs, h_kept_all.reshape(step_count * env_count, hidden)], axis=1)
    return (operand, grad_gates.reshape(step_count * env_count, 4 * hidden), head_grad, kl_part)

def reference(observations, physics_params, actions, reset_step, hidden_start, cell_start, old_logp, advantages, returns, lstm_weight, lstm_bias, head_weight):
    token_total = advantages.size
    adv_mean = jnp.sum(advantages) / token_total
    spread = jnp.sum((advantages - adv_mean) * (advantages - adv_mean)) / token_total
    norm_adv = (advantages - adv_mean) / jnp.sqrt(spread + spread_floor)
    env_total = observations.shape[1]
    env_block = math.gcd(env_total, 1024)
    block_count = env_total // env_block

    def take_block(source, block_index, axis_dim):
        return lax.dynamic_slice_in_dim(source, block_index * env_block, env_block, axis_dim)

    def add_block(running, block_index):
        operand, grad_gates, head_grad, kl_part = local_terms(take_block(observations, block_index, 1), take_block(physics_params, block_index, 0), take_block(actions, block_index, 1), take_block(reset_step, block_index, 0), take_block(hidden_start, block_index, 0), take_block(cell_start, block_index, 0), take_block(old_logp, block_index, 1), take_block(norm_adv, block_index, 1), take_block(returns, block_index, 1), lstm_weight, lstm_bias, head_weight)
        lstm_grad = lax.dot_general(operand, grad_gates, (((0,), (0,)), ((), ())), preferred_element_type=jnp.float32)
        bias_grad = lax.optimization_barrier(jnp.sum(grad_gates.astype(jnp.float32), axis=0))
        return ((running[0] + lstm_grad, running[1] + bias_grad, running[2] + head_grad, running[3] + kl_part), None)
    initial = (jnp.zeros(lstm_weight.shape, jnp.float32), jnp.zeros(lstm_bias.shape, jnp.float32), jnp.zeros(head_weight.shape, jnp.float32), jnp.zeros((), jnp.float32))
    running, unused = lax.scan(add_block, initial, jnp.arange(block_count, dtype=jnp.int32))
    param_total = lstm_weight.size + lstm_bias.size + head_weight.size
    grad_sq = jnp.sum(running[0] * running[0]) + jnp.sum(running[1] * running[1]) + jnp.sum(running[2] * running[2])
    scale = 1.0 / jnp.sqrt(grad_sq / param_total + 1.0)
    return (running[0] * scale, running[1] * scale, running[2] * scale, running[3] / token_total)
```

```python
import functools
import jax
import jax.numpy as jnp
from jax import lax
from jax.experimental import pallas as pl
from jax.experimental.pallas import tpu as pltpu
from jax.sharding import Mesh
from jax.sharding import PartitionSpec as P

F32 = jnp.float32
BF16 = jnp.bfloat16
VMEM = pl.BlockSpec(memory_space=pltpu.VMEM)
HIGH = lax.Precision.HIGHEST
ENV = ("env_0", "env_1", "env_2", "env_3")
CHIPS = ENV[:3]
CORE = ENV[3]
MIDDLE = 5.0

kl_coef = 0.5
value_coef = 0.5
spread_floor = 0.25


def forward_kernel(
    steps, envs, hidden, obs, phys, reset, h0, c0, w, bias,
    op_t, hseq, saved, w_t,
    x_in, proj, h_keep,
):
    width = x_in.shape[1]
    feats = obs.shape[2]
    for s in range(steps):
        x_in[s * envs : (s + 1) * envs, :feats] = obs[s]
        x_in[s * envs : (s + 1) * envs, feats:] = phys[...]
    block = 256
    for j in range(4 * hidden // block):
        cols = slice(j * block, (j + 1) * block)
        proj[:, cols] = (
            jnp.dot(x_in[...], w[:width, cols], preferred_element_type=F32) + bias[:, cols]
        )

    def step(s, c_prev):
        rows = pl.ds(pl.multiple_of(s * envs, envs), envs)
        before = pl.ds(pl.multiple_of(jnp.maximum(s - 1, 0) * envs, envs), envs)
        keep = reset[...] != s
        h_prev = jnp.where(s == 0, h0[...], hseq[before, :])
        h_kept = jnp.where(keep, h_prev.astype(F32), 0.0)
        h_keep[rows, :] = h_kept
        h_mul = h_kept.astype(BF16)
        c_kept = jnp.where(keep, c_prev, 0.0)
        c_next = []
        for j in range(hidden // block):
            here = slice(j * block, (j + 1) * block)
            pre = []
            for gate in range(4):
                cols = slice(gate * hidden + j * block, gate * hidden + (j + 1) * block)
                pre.append(
                    proj[rows, cols] + jnp.dot(h_mul, w[width:, cols], preferred_element_type=F32)
                )
            gate_i = jax.nn.sigmoid(pre[0])
            gate_f = jax.nn.sigmoid(pre[1])
            cand = jnp.tanh(pre[2])
            gate_o = jax.nn.sigmoid(pre[3])
            c_old = c_kept[:, here]
            c_new = gate_f * c_old + gate_i * cand
            tanh_c = jnp.tanh(c_new)
            hseq[rows, here] = (gate_o * tanh_c).astype(BF16)
            saved[0, rows, here] = cand * (gate_i * (1.0 - gate_i))
            saved[1, rows, here] = c_old * (gate_f * (1.0 - gate_f))
            saved[2, rows, here] = gate_i * (1.0 - cand * cand)
            saved[3, rows, here] = tanh_c * (gate_o * (1.0 - gate_o))
            saved[4, rows, here] = gate_o * (1.0 - tanh_c * tanh_c)
            saved[5, rows, here] = gate_f
            c_next.append(c_new)
        part = pl.ds(pl.multiple_of(s * block, block), block)
        w_t[part, :] = w[width:, part].T
        return jnp.concatenate(c_next, axis=1)

    lax.fori_loop(0, steps, step, c0[...])
    op_t[:width, :] = x_in[...].astype(F32).T
    for j in range(hidden // block):
        op_t[width + j * block : width + (j + 1) * block, :] = h_keep[
            :, j * block : (j + 1) * block
        ].T


def backward_kernel(
    steps, envs, hidden, acts, bins, kl_coef, value_coef,
    core, stats, reset, actions, old_logp, adv, returns, hseq, head_w, saved, w_t,
    kept, sent, head_own, kl_out,
    from_head,
):
    tokens = steps * envs
    width = head_w.shape[1]
    eye = (
        lax.broadcasted_iota(jnp.int32, (envs, envs), 0)
        == lax.broadcasted_iota(jnp.int32, (envs, envs), 1)
    ).astype(F32)

    def column(ref):
        return jnp.sum(ref[...][:, None, :] * eye[None], axis=2, keepdims=True).reshape(tokens, 1)

    norm_adv = (column(adv) - stats[0, 0]) * stats[0, 1]
    lane = lax.broadcasted_iota(jnp.int32, (1, width), 1)
    joint_of = lane // bins
    level_of = lane - joint_of * bins
    is_policy = lane < acts * bins
    spread = (
        (lax.broadcasted_iota(jnp.int32, (acts, width), 0) == joint_of) & is_policy
    ).astype(F32)
    logits = jnp.dot(hseq[...], head_w[...], preferred_element_type=F32)
    policy = jnp.where(is_policy, logits, 0.0)
    exp_policy = jnp.exp(policy)
    sum_exp = lax.dot_general(
        exp_policy, spread, (((1,), (1,)), ((), ())), precision=HIGH, preferred_element_type=F32
    )
    log_sum = jnp.sum(jnp.log(sum_exp), axis=1, keepdims=True)
    inverse = jnp.dot(1.0 / sum_exp, spread, precision=HIGH, preferred_element_type=F32)
    probs = exp_policy * inverse
    taken = jnp.dot(
        actions[...].astype(BF16), spread.astype(BF16), preferred_element_type=F32
    ).astype(jnp.int32)
    chosen = (taken == level_of) & is_policy
    token_logp = jnp.sum(jnp.where(chosen, policy, 0.0), axis=1, keepdims=True) - log_sum
    log_ratio = token_logp - column(old_logp)
    ratio = jnp.exp(log_ratio)
    kl_out[...] = jnp.sum(ratio - 1.0 - log_ratio, axis=0, keepdims=True)
    grad_logp = kl_coef * (ratio - 1.0) - norm_adv * ratio
    grad_policy = grad_logp * (jnp.where(chosen, 1.0, 0.0) - probs)
    grad_value = value_coef * (logits - column(returns))
    grad_logits = jnp.where(
        is_policy, grad_policy, jnp.where(lane == acts * bins, grad_value, 0.0)
    ).astype(BF16)
    first = core[0, 0] == 0
    head_sum = lax.dot_general(
        hseq[...], grad_logits, (((0,), (0,)), ((), ())), preferred_element_type=F32
    )
    left, right = head_sum[:, :128], head_sum[:, 128:]
    head_own[...] = jnp.where(first, left, right)
    other = jnp.where(first, right, left)
    for piece in range(hidden // tokens):
        spot = slice(2 * hidden + piece * 128, 2 * hidden + (piece + 1) * 128)
        sent[:, spot] = other[piece * tokens : (piece + 1) * tokens, :]
    from_head[...] = lax.dot_general(
        grad_logits, head_w[...], (((1,), (1,)), ((), ())), preferred_element_type=F32
    )

    def step(back, state):
        s = steps - 1 - back
        gh_next, gc_next = state
        rows = pl.ds(pl.multiple_of(s * envs, envs), envs)
        keep = reset[...] != s
        gh = from_head[rows, :] + gh_next
        gc = gc_next + gh * saved[4, rows, :]
        gates = [
            (gc * saved[0, rows, :]).astype(BF16),
            (gc * saved[1, rows, :]).astype(BF16),
            (gc * saved[2, rows, :]).astype(BF16),
            (gh * saved[3, rows, :]).astype(BF16),
        ]
        for k in range(2):
            cols = slice(k * hidden, (k + 1) * hidden)
            low, high = gates[k].astype(F32), gates[k + 2].astype(F32)
            kept[rows, cols] = jnp.where(first, low, high).astype(BF16)
            sent[rows, cols] = jnp.where(first, high, low)
        gh_prev = jnp.dot(jnp.concatenate(gates, axis=1), w_t[...], preferred_element_type=F32)
        gc_prev = gc * saved[5, rows, :]
        return jnp.where(keep, gh_prev, 0.0), jnp.where(keep, gc_prev, 0.0)

    zero = jnp.zeros((envs, hidden), F32)
    lax.fori_loop(0, steps, step, (zero, zero))


def gradient_kernel(
    hidden, chip_orders, pads,
    core, op_own, op_got, kept, got, head_own,
    *rest,
):
    outs, (lhs, mixed, gates) = rest[: len(chip_orders)], rest[len(chip_orders) :]
    tokens = kept.shape[0]
    half = kept.shape[1]
    rows_all = op_own.shape[0]
    chips = len(chip_orders[0])
    per_chip = rows_all // chips
    gates[:tokens, :] = kept[...]
    gates[tokens:, :] = got[:, :half].astype(BF16)
    start = 0
    for color, order in enumerate(chip_orders):
        out = outs[color]
        count = out.shape[1] - pads[color]
        if order == list(range(chips)):
            lhs[:, :tokens] = op_own[...].astype(BF16)
            lhs[:, tokens:] = op_got[...].astype(BF16)
        else:
            for place, chip in enumerate(order):
                to = slice(place * per_chip, (place + 1) * per_chip)
                of = slice(chip * per_chip, (chip + 1) * per_chip)
                mixed[to, :tokens] = op_own[of, :]
                mixed[to, tokens:] = op_got[of, :]
            lhs[...] = mixed[...].astype(BF16)
        done = 0
        while done < count:
            size = min(256, count - done)
            out[:, done : done + size] = jnp.dot(
                lhs[...], gates[:, start + done : start + done + size], preferred_element_type=F32
            )
            done += size
        start += count
    out = outs[0]
    spot = slice(out.shape[1] - pads[0], out.shape[1])
    out[:, spot] = jnp.zeros((rows_all, pads[0]), F32)
    quarter = tokens
    head_rows = head_own.shape[0] // chips
    for chip in range(chips):
        of = slice(chip * head_rows, (chip + 1) * head_rows)
        piece = (chip * head_rows) // quarter
        inner = chip * head_rows - piece * quarter
        out[chip * per_chip : chip * per_chip + head_rows, spot] = (
            head_own[of, :]
            + got[inner : inner + head_rows, half + piece * 128 : half + (piece + 1) * 128]
        )
    ones = jnp.ones((16, 2 * tokens), BF16)
    width = 2 * half // chips
    for block in range(half // 512):
        cols = slice(block * 512, (block + 1) * 512)
        sums = jnp.dot(ones, gates[:, cols], preferred_element_type=F32)[:1, :]
        for k in range(512 // width):
            chip = block * (512 // width) + k
            value = sums[:, k * width : (k + 1) * width]
            for side in range(2):
                row = (side * (chips // 2) + chip) * per_chip + head_rows
                out[row : row + 1, spot.start : spot.start + width] = jnp.where(
                    core[0, 0] == side, value, 0.0
                )


RIGHT = [(0, 1), (1, 2), (2, 3), (3, 0)]
LEFT = [(0, 3), (1, 0), (2, 1), (3, 2)]
ACROSS = [(0, 2), (1, 3), (2, 0), (3, 1)]
SWAP = [(0, 1), (1, 0)]


def pick(pieces, index):
    return lax.dynamic_index_in_dim(pieces, index, 0, keepdims=False)


def scatter_ring(array, axis):
    me = lax.axis_index(axis)
    pieces = array.reshape(4, array.shape[0] // 4, array.shape[1])
    right = lax.ppermute(pick(pieces, (me + 1) % 4), axis, RIGHT)
    left = lax.ppermute(pick(pieces, (me + 3) % 4), axis, LEFT)
    across = lax.ppermute(pick(pieces, (me + 2) % 4), axis, ACROSS)
    return (pick(pieces, me) + right) + (left + across)


def sum_everywhere(array):
    array = array + lax.ppermute(array, CORE, SWAP)
    for axis in CHIPS:
        right = lax.ppermute(array, axis, RIGHT)
        left = lax.ppermute(array, axis, LEFT)
        across = lax.ppermute(array, axis, ACROSS)
        array = (array + across) + (right + left)
    return array


def shards(
    observations, physics_params, actions, reset_step, hidden_start, cell_start,
    old_logp, advantages, returns, lstm_weight, lstm_bias, head_weight,
):
    steps, envs, _ = observations.shape
    hidden = hidden_start.shape[1]
    gate_cols = lstm_weight.shape[1]
    rows_all = lstm_weight.shape[0]
    width_in = rows_all - hidden
    tokens = steps * envs
    acts = actions.shape[2]
    head_cols = head_weight.shape[1]
    bins = (head_cols - 1) // acts
    half = gate_cols // 2
    token_total = advantages.size * lax.axis_size(ENV)
    core = lax.axis_index(CORE)
    core_in = core.astype(jnp.int32).reshape(1, 1)
    reset_in = reset_step[:, None]

    shifted = advantages - MIDDLE
    sums = sum_everywhere(
        jnp.stack([jnp.sum(shifted), jnp.sum(shifted * shifted)]).reshape(1, 2)
    )
    offset = sums[:, :1] / token_total
    spread = sums[:, 1:] / token_total - offset * offset
    stats = jnp.concatenate([offset + MIDDLE, 1.0 / jnp.sqrt(spread + spread_floor)], axis=1)

    op_t, hseq, saved, w_t = pl.pallas_call(
        functools.partial(forward_kernel, steps, envs, hidden),
        out_shape=[
            jax.ShapeDtypeStruct((rows_all, tokens), F32),
            jax.ShapeDtypeStruct((tokens, hidden), BF16),
            jax.ShapeDtypeStruct((6, tokens, hidden), F32),
            jax.ShapeDtypeStruct((gate_cols, hidden), BF16),
        ],
        in_specs=[VMEM] * 7,
        out_specs=[VMEM] * 4,
        scratch_shapes=[
            pltpu.VMEM((tokens, width_in), BF16),
            pltpu.VMEM((tokens, gate_cols), F32),
            pltpu.VMEM((tokens, hidden), F32),
        ],
        cost_estimate=pl.CostEstimate(
            flops=40_000_000_000, bytes_accessed=30_000_000, transcendentals=0
        ),
        name="forward",
    )(
        observations, physics_params, reset_in, hidden_start, cell_start,
        lstm_weight, lstm_bias.reshape(1, -1),
    )
    op_got = lax.ppermute(op_t, CORE, SWAP)
    head_pad = jnp.pad(head_weight, ((0, 0), (0, 256 - head_cols)))
    kept, sent, head_own, kl_part = pl.pallas_call(
        functools.partial(
            backward_kernel, steps, envs, hidden, acts, bins, kl_coef, value_coef
        ),
        out_shape=[
            jax.ShapeDtypeStruct((tokens, half), BF16),
            jax.ShapeDtypeStruct((tokens, half + 512), F32),
            jax.ShapeDtypeStruct((hidden, 128), F32),
            jax.ShapeDtypeStruct((1, 1), F32),
        ],
        in_specs=[pl.BlockSpec(memory_space=pltpu.SMEM)] * 2 + [VMEM] * 9,
        out_specs=[VMEM] * 4,
        scratch_shapes=[pltpu.VMEM((tokens, hidden), F32)],
        cost_estimate=pl.CostEstimate(
            flops=40_000_000_000, bytes_accessed=30_000_000, transcendentals=0
        ),
        name="backward",
    )(
        core_in, stats, reset_in, actions.reshape(tokens, acts), old_logp, advantages, returns,
        hseq, head_pad, saved, w_t,
    )
    got = lax.ppermute(sent, CORE, SWAP)

    sizes = [half - 768 - 640, 768, 640]
    pads = [128, 0, 0]
    orders = []
    for color in range(3):
        order = []
        for place in range(64):
            at = [0, 0, 0]
            for depth in range(3):
                at[(color + depth) % 3] = (place // (16, 4, 1)[depth]) % 4
            order.append(at[0] * 16 + at[1] * 4 + at[2])
        orders.append(order)
    parts = pl.pallas_call(
        functools.partial(gradient_kernel, hidden, orders, pads),
        out_shape=[
            jax.ShapeDtypeStruct((rows_all, size + pad), F32) for size, pad in zip(sizes, pads)
        ],
        in_specs=[pl.BlockSpec(memory_space=pltpu.SMEM)] + [VMEM] * 5,
        out_specs=[VMEM] * 3,
        scratch_shapes=[
            pltpu.VMEM((rows_all, 2 * tokens), BF16),
            pltpu.VMEM((rows_all, 2 * tokens), F32),
            pltpu.VMEM((2 * tokens, half), BF16),
        ],
        name="gradient",
    )(core_in, op_t, op_got, kept, got, head_own)
    parts = list(parts)
    for phase in range(3):
        for color in range(3):
            parts[color] = scatter_ring(parts[color], CHIPS[(color + phase) % 3])
    local_squares = sum(jnp.sum(part * part) for part in parts)
    totals = sum_everywhere(jnp.stack([local_squares, kl_part[0, 0]]).reshape(1, 2))

    each = rows_all // 128
    tile = parts[0][:, sizes[0] :]
    mine = jnp.concatenate([parts[0][:, : sizes[0]], parts[1], parts[2]], axis=1)
    pair = mine.reshape(2, each, half)
    parcel = jnp.concatenate([pick(pair, 1 - core), tile.reshape(each, -1)], axis=1)
    parcel = lax.ppermute(parcel, CORE, SWAP)
    tile_got = parcel[:, half:].reshape(tile.shape)
    first = core == 0

    def in_order(own, other):
        return jnp.concatenate(
            [jnp.where(first, own, other), jnp.where(first, other, own)], axis=1
        )

    param_total = lstm_weight.size + lstm_bias.size + head_weight.size
    scale = 1.0 / jnp.sqrt(totals[0, 0] / param_total + 1.0)
    lstm_part = in_order(pick(pair, core), parcel[:, :half]) * scale
    head_rows = 8
    head_at = core * head_rows
    head_part = in_order(
        lax.dynamic_slice_in_dim(tile, head_at, head_rows, 0),
        lax.dynamic_slice_in_dim(tile_got, head_at, head_rows, 0),
    )[:, :head_cols] * scale
    bias_row = (tile + tile_got)[2 * head_rows, :64].reshape(2, 32)
    bias_part = pick(bias_row, core) * scale
    return (lstm_part, bias_part, head_part, totals[0, 1] / token_total)


def solution(mesh):
    split = Mesh(mesh.devices.reshape(4, 4, 4, 2), ENV)
    return jax.shard_map(
        shards,
        mesh=split,
        in_specs=(
            P(None, ENV, None), P(ENV, None), P(None, ENV, None), P(ENV), P(ENV, None),
            P(ENV, None), P(None, ENV), P(None, ENV), P(None, ENV), P(), P(), P(),
        ),
        out_specs=(P(ENV, None), P(ENV), P(ENV, None), P()),
        check_vma=False,
    )
```
